16 devices in a mesh: depth: 2 (over z), col: 2 (over y), row: 4 (over x, core).
Axes of the slice: x: 2, y: 2, z: 2, core: 2. Of those that a mesh axis runs over, the one named last changes fastest.
Arguments:
- tokens: bfloat16 [32768, 1280], P(('depth', 'row'), 'col')
- w_up: bfloat16 [1280, 5120], P('row', 'col')
- w_down: bfloat16 [5120, 1280], P('row', 'col')
- w_value: bfloat16 [1280, 1280], P('row', 'col')
- w_output: bfloat16 [1280, 1280], P('row', 'col')
- grad_out: bfloat16 [32768, 1280], P(('depth', 'row'), 'col')
Outputs:
- output 1: bfloat16 [32768, 1280], P(('depth', 'row'), 'col')
- output 2: bfloat16 [32768, 1280], P(('depth', 'row'), 'col')
- output 3: float32 [1280, 5120], P('row', 'col')
- output 4: float32 [5120, 1280], P('row', 'col')
- output 5: float32 [1280, 1280], P('row', 'col')
- output 6: float32 [1280, 1280], P('row', 'col')
All inputs are finite; a program needn't handle non-finite values.
Results may differ from the reference program's by a relative error of at most 0.001.
Values are sent between devices in bfloat16 or wider.
A program may use at most 1 GiB of HBM per device.

```python
import jax
import jax.numpy as jnp
from jax import lax

TOK_DEV = 4096
D = 1280
FF = 5120
TOKENS = 32768


def setup_inputs(seed: int = 0) -> dict:
    key_list = jax.random.split(jax.random.key(seed), 6)
    tokens = jax.random.normal(key_list[0], (TOKENS, D), jnp.float32)
    w_up = jax.random.normal(key_list[1], (D, FF), jnp.float32) * D ** -0.5
    w_down = jax.random.normal(key_list[2], (FF, D), jnp.float32) * FF ** -0.5
    w_value = jax.random.normal(key_list[3], (D, D), jnp.float32) * D ** -0.5
    w_output = jax.random.normal(key_list[4], (D, D), jnp.float32) * D ** -0.5
    grad_out = jax.random.normal(key_list[5], (TOKENS, D), jnp.float32)
    return {
        "tokens": tokens.astype(jnp.bfloat16),
        "w_up": w_up.astype(jnp.bfloat16),
        "w_down": w_down.astype(jnp.bfloat16),
        "w_value": w_value.astype(jnp.bfloat16),
        "w_output": w_output.astype(jnp.bfloat16),
        "grad_out": grad_out.astype(jnp.bfloat16),
    }


def reference(tokens, w_up, w_down, w_value, w_output, grad_out):
    block_count = TOKENS // TOK_DEV

    def block_step(acc_carry, blk_pair):
        x_blk, g_blk = blk_pair
        pre_act = jnp.dot(x_blk, w_up, preferred_element_type=jnp.float32)
        act_f32, gelu_pull = jax.vjp(jax.nn.gelu, pre_act)
        act_bf16 = act_f32.astype(jnp.bfloat16)
        val_proj = jnp.dot(x_blk, w_value, preferred_element_type=jnp.float32).astype(jnp.bfloat16)
        y_blk = (jnp.dot(act_bf16, w_down, preferred_element_type=jnp.float32)
                 + jnp.dot(val_proj, w_output, preferred_element_type=jnp.float32)).astype(jnp.bfloat16)
        d_act = jnp.dot(g_blk, w_down.T, preferred_element_type=jnp.float32)
        d_pre = gelu_pull(d_act)[0].astype(jnp.bfloat16)
        d_val = jnp.dot(g_blk, w_output.T, preferred_element_type=jnp.float32).astype(jnp.bfloat16)
        dx_blk = (jnp.dot(d_pre, w_up.T, preferred_element_type=jnp.float32)
                  + jnp.dot(d_val, w_value.T, preferred_element_type=jnp.float32)).astype(jnp.bfloat16)
        acc_up, acc_down, acc_value, acc_output = acc_carry
        acc_up = acc_up + jnp.dot(x_blk.T, d_pre, preferred_element_type=jnp.float32)
        acc_down = acc_down + jnp.dot(act_bf16.T, g_blk, preferred_element_type=jnp.float32)
        acc_value = acc_value + jnp.dot(x_blk.T, d_val, preferred_element_type=jnp.float32)
        acc_output = acc_output + jnp.dot(val_proj.T, g_blk, preferred_element_type=jnp.float32)
        return (acc_up, acc_down, acc_value, acc_output), (y_blk, dx_blk)

    grad_init = (
        jnp.zeros((D, FF), jnp.float32),
        jnp.zeros((FF, D), jnp.float32),
        jnp.zeros((D, D), jnp.float32),
        jnp.zeros((D, D), jnp.float32),
    )
    blk_pairs = (tokens.reshape(block_count, TOK_DEV, D), grad_out.reshape(block_count, TOK_DEV, D))
    grad_sums, block_outs = lax.scan(block_step, grad_init, blk_pairs)
    y_out = block_outs[0].reshape(TOKENS, D)
    grad_in = block_outs[1].reshape(TOKENS, D)
    return (y_out, grad_in, grad_sums[0], grad_sums[1], grad_sums[2], grad_sums[3])
```

```python
import functools

import jax
import jax.numpy as jnp
from jax import lax
from jax.experimental import pallas as pl
from jax.experimental.pallas import tpu as pltpu
from jax.sharding import PartitionSpec as P

F32 = jnp.float32
BF16 = jnp.bfloat16
VMEM_LIMIT = 60 * 1024 * 1024

PERM_X = [(0, 2), (2, 0), (1, 3), (3, 1)]
PERM_CORE = [(0, 1), (1, 0), (2, 3), (3, 2)]
PERM_TWO = [(0, 1), (1, 0)]


def over_x(a):
    return lax.ppermute(a, "row", PERM_X)


def over_core(a):
    return lax.ppermute(a, "row", PERM_CORE)


def over_y(a):
    return lax.ppermute(a, "col", PERM_TWO)


def over_z(a):
    return lax.ppermute(a, "depth", PERM_TWO)


def dot_nn(a, b):
    return lax.dot_general(a, b, (((1,), (0,)), ((), ())), preferred_element_type=F32)


def dot_nt(a, b):
    return lax.dot_general(a, b, (((1,), (1,)), ((), ())), preferred_element_type=F32)


def dot_tn(a, b):
    return lax.dot_general(a, b, (((0,), (0,)), ((), ())), preferred_element_type=F32)


def take(a, idx, size, axis):
    return lax.dynamic_slice_in_dim(a, idx * size, size, axis)


def params():
    return pltpu.CompilerParams(dimension_semantics=("arbitrary",), vmem_limit_bytes=VMEM_LIMIT)


def tile_of(rows):
    return 512 if rows % 512 == 0 else rows


GELU_C = 0.7978845608028654
GELU_K = 0.044715


def act_kernel(x0, x1, g, w1, w2, a0, a1, d0, d1):
    half = x0.shape[1]
    n = w1.shape[1] // 2
    for out_a, out_d, lo in ((a0, d0, 0), (a1, d1, n)):
        u = dot_nn(x0[...], w1[:half, lo:lo + n]) + dot_nn(x1[...], w1[half:, lo:lo + n])
        da = dot_nt(g[...], w2[lo:lo + n, :])
        u2 = u * u
        t = jnp.tanh(GELU_C * (u * (1.0 + GELU_K * u2)))
        cdf = 0.5 * (1.0 + t)
        out_a[...] = (u * cdf).astype(BF16)
        slope = cdf + (0.5 * u * (1.0 - t * t)) * GELU_C * (1.0 + (3.0 * GELU_K) * u2)
        out_d[...] = (slope * da).astype(BF16)


def activations(x0, x1, g, w1, w2):
    rows, half = x0.shape
    full = g.shape[1]
    n = w1.shape[1] // 2
    tm = tile_of(rows)
    row_spec = lambda width: pl.BlockSpec((tm, width), lambda i: (i, 0))
    whole = lambda a: pl.BlockSpec(a.shape, lambda i: (0, 0))
    out = jax.ShapeDtypeStruct((rows, n), BF16)
    return pl.pallas_call(
        act_kernel,
        grid=(rows // tm,),
        in_specs=[row_spec(half), row_spec(half), row_spec(full), whole(w1), whole(w2)],
        out_specs=[row_spec(n)] * 4,
        out_shape=[out] * 4,
        compiler_params=params(),
        cost_estimate=pl.CostEstimate(
            flops=2 * rows * full * 2 * n * 2, transcendentals=rows * 2 * n,
            bytes_accessed=2 * (2 * rows * full + 2 * full * 2 * n + 4 * rows * n)),
        name="act",
    )(x0, x1, g, w1, w2)


def mm_kernel(plan, n_l, n_r, has_add, split, *refs):
    ls, rs = refs[:n_l], refs[n_l:n_l + n_r]
    outs = refs[n_l + n_r + has_add:]
    acc = refs[n_l + n_r][...] if has_add else None
    for li, ri, lo, hi, trans in plan:
        a = ls[li][...]
        term = dot_nt(a, rs[ri][:, lo:hi]) if trans else dot_nn(a, rs[ri][lo:hi, :])
        acc = term if acc is None else acc + term
    width = acc.shape[1] // split
    for i, o in enumerate(outs):
        o[...] = acc[:, i * width:(i + 1) * width].astype(o.dtype)


def multi_mm(name, plan, ls, rs, rows, offset, out_dtype, split=1, add=None):
    tm = tile_of(rows)
    cols = next(rs[ri].shape[0] if trans else rs[ri].shape[1] for _, ri, _, _, trans in plan)
    specs = []
    for a in ls:
        off = offset // tm if a.shape[0] > rows else 0
        specs.append(pl.BlockSpec((tm, a.shape[1]), functools.partial(lambda o, i: (i + o, 0), off)))
    specs += [pl.BlockSpec(b.shape, lambda i: (0, 0)) for b in rs]
    args = list(ls) + list(rs)
    if add is not None:
        specs.append(pl.BlockSpec((tm, cols), lambda i: (i, 0)))
        args.append(add)
    width = cols // split
    k_total = sum(hi - lo for _, _, lo, hi, _ in plan)
    return pl.pallas_call(
        functools.partial(mm_kernel, plan, len(ls), len(rs), int(add is not None), split),
        grid=(rows // tm,),
        in_specs=specs,
        out_specs=[pl.BlockSpec((tm, width), lambda i: (i, 0))] * split,
        out_shape=[jax.ShapeDtypeStruct((rows, width), out_dtype)] * split,
        compiler_params=params(),
        cost_estimate=pl.CostEstimate(
            flops=2 * rows * cols * k_total, transcendentals=0,
            bytes_accessed=2 * rows * k_total + 2 * cols * k_total + 4 * rows * cols),
        name=name,
    )(*args)


def solution(mesh):
    act_spec = P(("depth", "row"), "col")
    wgt_spec = P("row", "col")

    def device_step(x_blk, w1_blk, w2_blk, wv_blk, wo_blk, g_blk):
        row = lax.axis_index("row")
        x, c = row // 2, row % 2
        y, z = lax.axis_index("col"), lax.axis_index("depth")
        same = x == y

        def pair(pred, a, b):
            return jnp.where(pred, a, b), jnp.where(pred, b, a)

        rows, half = x_blk.shape
        mine = rows // 2
        full = 2 * half
        vrow = wv_blk.shape[0]
        ff_blk = w2_blk.shape[0]
        quart = ff_blk // 2
        unit = quart // 5
        chunks = [(0, 2 * unit), (2 * unit, 4 * unit), (4 * unit, 5 * unit)]

        xa, ga = take(x_blk, y, mine, 0), take(g_blk, y, mine, 0)
        xb = over_y(take(x_blk, 1 - y, mine, 0))
        wv_y, wo_y = over_y(wv_blk), over_y(wo_blk)
        gb = over_y(take(g_blk, 1 - y, mine, 0))
        xao, xbo, gao, gbo = over_core(xa), over_core(xb), over_core(ga), over_core(gb)
        x0m, x1m = pair(same, xa, xb)
        x0o, x1o = pair(same, xao, xbo)
        x0, x1 = jnp.concatenate([x0m, x0o], 0), jnp.concatenate([x1m, x1o], 0)
        g = jnp.concatenate([jnp.concatenate([ga, gb], 1), jnp.concatenate([gao, gbo], 1)], 0)

        wv_own = jnp.concatenate(pair(y == 0, wv_blk, wv_y), 1)
        wv_xn = over_x(wv_own)
        wv_oc = over_core(jnp.concatenate([wv_own, wv_xn], 0))
        wv0 = jnp.concatenate(pair(c == 0, wv_own, wv_oc[:vrow]), 0)
        wv1 = jnp.concatenate(pair(c == 0, wv_xn, wv_oc[vrow:]), 0)
        wo_own = jnp.concatenate([wo_blk, wo_y], 1)
        wo_xn = over_x(wo_own)
        wo_oc = over_core(jnp.concatenate([wo_own, wo_xn], 0))
        wo_near = jnp.concatenate(pair(c == 0, wo_own, wo_oc[:vrow]), 0)
        wo_far = jnp.concatenate(pair(c == 0, wo_xn, wo_oc[vrow:]), 0)
        wo_full = jnp.concatenate(pair(x == 0, wo_near, wo_far), 0)

        w1_keep = take(w1_blk, c, ff_blk, 1)
        w1_oc = over_core(take(w1_blk, 1 - c, ff_blk, 1))
        q1 = jnp.concatenate(pair(c == 0, w1_keep, w1_oc), 0)
        q1_m, q1_o = take(q1, z, quart, 1), take(q1, 1 - z, quart, 1)
        q2_m, q2_o = take(w2_blk, z, quart, 0), take(w2_blk, 1 - z, quart, 0)
        w1s, w2s = [], []
        for lo, hi in chunks:
            w = hi - lo
            a1, a2 = q1_m[:, lo:hi], q2_m[lo:hi]
            b1, b2 = over_y(a1), over_y(a2)
            n1 = over_x(jnp.concatenate([a1, b1], 1))
            n2 = over_x(jnp.concatenate([a2, b2], 1))
            fb1, fn1, fb2, fn2 = over_z(b1), over_z(n1), over_z(b2), over_z(n2)
            fa1, fa2 = q1_o[:, lo:hi], q2_o[lo:hi]
            near = pair(same, a1, b1), pair(same, fa1, fb1)
            far = pair(same, n1[:, :w], n1[:, w:]), pair(same, fn1[:, :w], fn1[:, w:])
            w1s.append(jnp.concatenate([
                jnp.concatenate([near[0][0], near[1][0], near[0][1], near[1][1]], 1),
                jnp.concatenate([far[0][0], far[1][0], far[0][1], far[1][1]], 1)], 0))
            w2s.append(jnp.concatenate([
                jnp.concatenate([a2, b2], 1), jnp.concatenate([fa2, fb2], 1), n2, fn2], 0))

        v, = multi_mm("val", [(0, 0, 0, half, False), (1, 1, 0, half, False)],
                      [x0, x1], [wv0, wv1], mine, 0, BF16)
        dv, = multi_mm("dval", [(0, 0, 0, full, True)], [g], [wo_full], mine, 0, BF16)

        def core_half(a):
            blk = a.reshape(2, 2, vrow, full)
            send = take(blk, 1 - c, 1, 1)[:, 0]
            keep = take(blk, c, 1, 1)[:, 0]
            return keep + over_core(send)

        pv = core_half(jnp.concatenate([dot_tn(x0[:mine], dv), dot_tn(x1[:mine], dv)], 0))
        pv = take(pv, y, half, 2) + over_y(take(pv, 1 - y, half, 2))
        pv = pv[0] + over_x(pv[1])
        grad_value = pv + over_z(pv)
        po = core_half(dot_tn(v, g[:mine]))
        po = po[:, :, :half] + over_y(po[:, :, half:])
        po = take(po, x, 1, 0)[0] + over_x(take(po, 1 - x, 1, 0)[0])
        grad_output = po + over_z(po)

        acts, dacts, up_parts, down_parts = [], [], [], []
        for w1c, w2c, (lo, hi) in zip(w1s, w2s, chunks):
            w = hi - lo
            a0, a1, d0, d1 = activations(x0, x1, g, w1c, w2c)
            acts.append((a0, a1))
            dacts.append((d0, d1))
            s = jnp.concatenate([dot_tn(x0, d0), dot_tn(x0, d1)], 1)
            s = s + over_x(jnp.concatenate([dot_tn(x1, d1), dot_tn(x1, d0)], 1))
            s = s.reshape(half, 2, 2, w)
            s = s[:, :, 0] + over_z(s[:, :, 1])
            keep, send = pair(same, s[:, 0], s[:, 1])
            s = keep + over_y(send)
            s_m = take(s, c, vrow, 0)
            s_o = over_core(take(s, 1 - c, vrow, 0))
            up_parts.append((s_m, s_o, over_z(s_m), over_z(s_o)))
            s = dot_tn(a0, g) + over_x(dot_tn(a1, g))
            s = s[:w] + over_z(s[w:])
            s = s[:, :half] + over_y(s[:, half:])
            down_parts.append((s, over_z(s)))

        def hidden_order(which):
            near = jnp.concatenate([p[which[0]] for p in up_parts], 1)
            far = jnp.concatenate([p[which[1]] for p in up_parts], 1)
            return jnp.concatenate(pair(z == 0, near, far), 1)

        grad_up = jnp.concatenate(pair(c == 0, hidden_order((0, 2)), hidden_order((1, 3))), 1)
        grad_down = jnp.concatenate(pair(
            z == 0, jnp.concatenate([p[0] for p in down_parts], 0),
            jnp.concatenate([p[1] for p in down_parts], 0)), 0)

        n_c = len(chunks)
        y_plan, x_plan = [], []
        for k, (lo, hi) in enumerate(chunks):
            n = 2 * (hi - lo)
            for b in range(2):
                y_plan.append((2 * k + b, k, b * n, (b + 1) * n, False))
                x_plan.append((2 * k + b, k, b * n, (b + 1) * n, True))
        a_list = [a for p in acts for a in p]
        d_list = [d for p in dacts for d in p]
        y_o, = multi_mm("yfar", y_plan, a_list, w2s, mine, mine, F32)
        x_o, = multi_mm("xfar", x_plan, d_list, w1s, mine, mine, F32)
        y_r, x_r = over_core(y_o), over_core(x_o)
        wv_t = jnp.concatenate([wv0, wv1], 0)
        ya, yb = multi_mm("ynear", y_plan + [(2 * n_c, n_c, 0, full, False)],
                          a_list + [v], w2s + [wo_full], mine, 0, BF16, split=2, add=y_r)
        da, db = multi_mm("xnear", x_plan + [(2 * n_c, n_c, 0, full, True)],
                          d_list + [dv], w1s + [wv_t], mine, 0, BF16, split=2, add=x_r)
        da, db = pair(same, da, db)
        y_out = jnp.concatenate(pair(y == 0, ya, over_y(yb)), 0)
        grad_in = jnp.concatenate(pair(y == 0, da, over_y(db)), 0)
        return y_out, grad_in, grad_up, grad_down, grad_value, grad_output

    return jax.shard_map(
        device_step,
        mesh=mesh,
        in_specs=(act_spec, wgt_spec, wgt_spec, wgt_spec, wgt_spec, act_spec),
        out_specs=(act_spec, act_spec, wgt_spec, wgt_spec, wgt_spec, wgt_spec),
        check_vma=False,
    )
```

```python
import functools

import jax
import jax.numpy as jnp
from jax import lax
from jax.experimental import pallas as pl
from jax.experimental.pallas import tpu as pltpu
from jax.sharding import PartitionSpec as P


F32 = jnp.float32
BF16 = jnp.bfloat16
VMEM_LIMIT = 60 * 1024 * 1024

PERM_X = [(0, 2), (2, 0), (1, 3), (3, 1)]
PERM_CORE = [(0, 1), (1, 0), (2, 3), (3, 2)]
PERM_TWO = [(0, 1), (1, 0)]


def over_x(a):
    return lax.ppermute(a, "row", PERM_X)


def over_core(a):
    return lax.ppermute(a, "row", PERM_CORE)


def over_y(a):
    return lax.ppermute(a, "col", PERM_TWO)


def over_z(a):
    return lax.ppermute(a, "depth", PERM_TWO)


def dot_nn(a, b):
    return lax.dot_general(a, b, (((1,), (0,)), ((), ())), preferred_element_type=F32)


def dot_nt(a, b):
    return lax.dot_general(a, b, (((1,), (1,)), ((), ())), preferred_element_type=F32)


def dot_tn(a, b):
    return lax.dot_general(a, b, (((0,), (0,)), ((), ())), preferred_element_type=F32)


def take(a, idx, size, axis):
    return lax.dynamic_slice_in_dim(a, idx * size, size, axis)


def params():
    return pltpu.CompilerParams(dimension_semantics=("arbitrary",), vmem_limit_bytes=VMEM_LIMIT)


def tile_of(rows):
    return 512 if rows % 512 == 0 else rows


GELU_C = 0.7978845608028654
GELU_K = 0.044715


def col_blocks(q):
    cut = q - q % 256
    return [(0, cut), (cut, 2 * q - cut), (2 * q - cut, 2 * q)] if q % 256 else [(0, q), (q, 2 * q)]


def by_block(lo, hi, q):
    return [(b, max(lo, b * q), min(hi, (b + 1) * q)) for b in range(2) if max(lo, b * q) < min(hi, (b + 1) * q)]


def gelu_kernel(n_prev, x, w1, *refs):
    s_h0, s_h1, a_0, a_1 = refs[n_prev:]
    q = w1.shape[1] // 4
    for h, out_s in enumerate((s_h0, s_h1)):
        for lo, hi in col_blocks(q):
            u = dot_nn(x[...], w1[:, 2 * h * q + lo:2 * h * q + hi])
            u2 = u * u
            cdf = 0.5 + 0.5 * jnp.tanh(u * (GELU_C + (GELU_C * GELU_K) * u2))
            a = u * cdf
            out_s[:, lo:hi] = cdf + (a - a * cdf) * (2.0 * GELU_C + (6.0 * GELU_C * GELU_K) * u2)
            a = a.astype(BF16)
            for b, f, t in by_block(lo, hi, q):
                (a_0, a_1)[b][:, h * q + f - b * q:h * q + t - b * q] = a[:, f - lo:t - lo]


def gelu_call(x, w1, rows, offset, prev):
    tm = tile_of(rows)
    off = offset // tm
    at = lambda i: (i + off, 0)
    q = w1.shape[1] // 4
    widths = [(2 * q, F32), (2 * q, F32), (2 * q, BF16), (2 * q, BF16)]
    return pl.pallas_call(
        functools.partial(gelu_kernel, len(prev)),
        grid=(rows // tm,),
        in_specs=[pl.BlockSpec((tm, x.shape[1]), at), pl.BlockSpec(w1.shape, lambda i: (0, 0))]
        + [pl.BlockSpec(memory_space=pl.ANY)] * len(prev),
        out_specs=[pl.BlockSpec((tm, w), at) for w, _ in widths],
        out_shape=[jax.ShapeDtypeStruct((x.shape[0], w), d) for w, d in widths],
        input_output_aliases={2 + i: i for i in range(len(prev))},
        compiler_params=params(),
        cost_estimate=pl.CostEstimate(
            flops=2 * rows * w1.size, transcendentals=rows * 4 * q, bytes_accessed=rows * 4 * q * 8),
    )(x, w1, *prev)


def dgelu_kernel(g, slope, w2_b0, w2_b1, d):
    q = w2_b0.shape[0]
    for lo, hi in col_blocks(q):
        w2 = [(w2_b0, w2_b1)[b][f - b * q:t - b * q, :] for b, f, t in by_block(lo, hi, q)]
        da = dot_nt(g[...], w2[0] if len(w2) == 1 else jnp.concatenate(w2, 0))
        d[:, lo:hi] = (slope[:, lo:hi] * da).astype(BF16)


def token_call(body, tiled, weights, outs, k_total):
    rows = tiled[0].shape[0]
    tm = tile_of(rows)
    row_spec = lambda width: pl.BlockSpec((tm, width), lambda i: (i, 0))
    return pl.pallas_call(
        body,
        grid=(rows // tm,),
        in_specs=[row_spec(a.shape[1]) for a in tiled] + [
            pl.BlockSpec((n, a.shape[1]), functools.partial(lambda b, i: (b, 0), b)) for a, n, b in weights],
        out_specs=[row_spec(width) for width, _ in outs],
        out_shape=[jax.ShapeDtypeStruct((rows, width), dt) for width, dt in outs],
        compiler_params=params(),
        cost_estimate=pl.CostEstimate(
            flops=2 * rows * k_total * 1280, transcendentals=rows * k_total,
            bytes_accessed=rows * k_total * 8),
    )(*tiled, *[a for a, _, _ in weights])


def place_kernel(plan, flag, *refs):
    outs = refs[len(plan):]
    sure = flag[0] == 1
    for ref, (o, yes, no) in zip(refs, plan):
        r, c = ref.shape
        if yes == no:
            outs[o][yes[0]:yes[0] + r, yes[1]:yes[1] + c] = ref[...]
            continue

        @pl.when(sure)
        def _(ref=ref, o=o, at=yes, r=r, c=c):
            outs[o][at[0]:at[0] + r, at[1]:at[1] + c] = ref[...]

        @pl.when(jnp.logical_not(sure))
        def _(ref=ref, o=o, at=no, r=r, c=c):
            outs[o][at[0]:at[0] + r, at[1]:at[1] + c] = ref[...]


def place(shapes, pieces, plan, flag):
    vm = pl.BlockSpec(memory_space=pltpu.VMEM)
    return pl.pallas_call(
        functools.partial(place_kernel, plan),
        in_specs=[pl.BlockSpec(memory_space=pltpu.SMEM)] + [vm] * len(pieces),
        out_specs=[vm] * len(shapes),
        out_shape=[jax.ShapeDtypeStruct(s, BF16) for s in shapes],
        compiler_params=pltpu.CompilerParams(vmem_limit_bytes=VMEM_LIMIT),
        cost_estimate=pl.CostEstimate(flops=10 ** 9, transcendentals=0, bytes_accessed=10 ** 7),
    )(flag.astype(jnp.int32).reshape(1), *pieces)


def join_x_kernel(flag, a, b, ao, bo, whole):
    near = pl.program_id(0) < pl.num_programs(0) // 2
    same = flag[0] == 1

    def put(first, second):
        half = a.shape[1]

        @pl.when(same)
        def _():
            whole[:, :half] = first[...]
            whole[:, half:] = second[...]

        @pl.when(jnp.logical_not(same))
        def _():
            whole[:, :half] = second[...]
            whole[:, half:] = first[...]

    @pl.when(near)
    def _():
        put(a, b)

    @pl.when(jnp.logical_not(near))
    def _():
        put(ao, bo)


def join_g_kernel(a, b, ao, bo, g):
    near = pl.program_id(0) < pl.num_programs(0) // 2
    half = a.shape[1]

    @pl.when(near)
    def _():
        g[:, :half] = a[...]
        g[:, half:] = b[...]

    @pl.when(jnp.logical_not(near))
    def _():
        g[:, :half] = ao[...]
        g[:, half:] = bo[...]


def join(body, pieces, out_widths, flag=None):
    mine, half = pieces[0].shape
    tm = tile_of(mine)
    n = mine // tm
    first = pl.BlockSpec((tm, half), lambda i: (jnp.minimum(i, n - 1), 0))
    second = pl.BlockSpec((tm, half), lambda i: (jnp.maximum(i - n, 0), 0))
    specs, args = [first, first, second, second], list(pieces)
    if flag is not None:
        specs, args = [pl.BlockSpec(memory_space=pltpu.SMEM)] + specs, [flag] + args
    return pl.pallas_call(
        body,
        grid=(2 * n,),
        in_specs=specs,
        out_specs=[pl.BlockSpec((tm, width), lambda i: (i, 0)) for width in out_widths],
        out_shape=[jax.ShapeDtypeStruct((2 * mine, width), BF16) for width in out_widths],
        compiler_params=params(),
        cost_estimate=pl.CostEstimate(flops=mine * half * 1000, transcendentals=0, bytes_accessed=16 * mine * half),
    )(*args)


def mm_kernel(plan, n_l, n_r, has_add, split, *refs):
    ls, rs = refs[:n_l], refs[n_l:n_l + n_r]
    outs = refs[n_l + n_r + has_add:]
    acc = refs[n_l + n_r][...] if has_add else None
    for l_ids, ri, trans in plan:
        a = jnp.concatenate([ls[i][...] for i in l_ids], 1) if len(l_ids) > 1 else ls[l_ids[0]][...]
        term = dot_nt(a, rs[ri][...]) if trans else dot_nn(a, rs[ri][...])
        acc = term if acc is None else acc + term
    width = acc.shape[1] // split
    for i, o in enumerate(outs):
        o[...] = acc[:, i * width:(i + 1) * width].astype(o.dtype)


def multi_mm(plan, ls, rs, rows, offset, out_dtype, split=1, add=None):
    tm = tile_of(rows)
    cols = rs[0].shape[0] if plan[0][2] else rs[0].shape[1]
    specs = []
    for a in ls:
        off = offset // tm if a.shape[0] > rows else 0
        specs.append(pl.BlockSpec((tm, a.shape[1]), functools.partial(lambda o, i: (i + o, 0), off)))
    specs += [pl.BlockSpec(b.shape, lambda i: (0, 0)) for b in rs]
    args = list(ls) + list(rs)
    if add is not None:
        specs.append(pl.BlockSpec((tm, cols), lambda i: (i, 0)))
        args.append(add)
    width = cols // split
    k_total = sum(b.size // cols for b in rs)
    return pl.pallas_call(
        functools.partial(mm_kernel, plan, len(ls), len(rs), int(add is not None), split),
        grid=(rows // tm,),
        in_specs=specs,
        out_specs=[pl.BlockSpec((tm, width), lambda i: (i, 0))] * split,
        out_shape=[jax.ShapeDtypeStruct((rows, width), out_dtype)] * split,
        compiler_params=params(),
        cost_estimate=pl.CostEstimate(
            flops=2 * rows * cols * k_total, transcendentals=0,
            bytes_accessed=2 * rows * k_total + 2 * cols * k_total + 4 * rows * cols),
    )(*args)


def solution(mesh):
    act_spec = P(("depth", "row"), "col")
    wgt_spec = P("row", "col")

    def device_step(x_blk, w1_blk, w2_blk, wv_blk, wo_blk, g_blk):
        row = lax.axis_index("row")
        x, c = row // 2, row % 2
        y, z = lax.axis_index("col"), lax.axis_index("depth")
        same = x == y

        def pair(pred, a, b):
            return jnp.where(pred, a, b), jnp.where(pred, b, a)

        def cat(parts, axis):
            return jnp.concatenate(list(parts), axis)

        rows, half = x_blk.shape
        mine = rows // 2
        full = 2 * half
        vrow = wv_blk.shape[0]
        ff_blk = w2_blk.shape[0]
        q = ff_blk // 2

        xa, ga = take(x_blk, y, mine, 0), take(g_blk, y, mine, 0)
        xb = over_y(take(x_blk, 1 - y, mine, 0))
        gb = over_y(take(g_blk, 1 - y, mine, 0))
        xao, gao = over_core(xa), over_core(ga)
        xbo, gbo = over_core(xb), over_core(gb)

        w1_keep = take(w1_blk, c, ff_blk, 1)
        w1_oc = over_core(take(w1_blk, 1 - c, ff_blk, 1))
        q1 = cat(pair(c == 0, w1_keep, w1_oc), 0)
        a1, fa1 = take(q1, z, q, 1), take(q1, 1 - z, q, 1)
        a2, fa2 = take(w2_blk, z, q, 0), take(w2_blk, 1 - z, q, 0)
        b1, b2 = over_y(a1), over_y(a2)
        na1, nb1 = over_x(a1), over_x(b1)
        na2, nb2 = over_x(a2), over_x(b2)
        fb1, fna1, fnb1 = over_z(b1), over_z(na1), over_z(nb1)
        fb2, fna2, fnb2 = over_z(b2), over_z(na2), over_z(nb2)

        wv_y, wo_y = over_y(wv_blk), over_y(wo_blk)
        wv_own = cat(pair(y == 0, wv_blk, wv_y), 1)
        wv_xn = over_x(wv_own)
        wv_oc, wv_xc = over_core(wv_own), over_core(wv_xn)
        wo_own = cat([wo_blk, wo_y], 1)
        wo_xn = over_x(wo_own)
        wo_oc, wo_xc = over_core(wo_own), over_core(wo_xn)
        wv_full = cat([cat(pair(c == 0, wv_own, wv_oc), 0), cat(pair(c == 0, wv_xn, wv_xc), 0)], 0)
        wo_near = cat(pair(c == 0, wo_own, wo_oc), 0)
        wo_far = cat(pair(c == 0, wo_xn, wo_xc), 0)
        wo_full = cat(pair(x == 0, wo_near, wo_far), 0)

        plan1, pieces1 = [], []
        for r, group in enumerate(((a1, b1, fa1, fb1), (na1, nb1, fna1, fnb1))):
            for i, piece in enumerate(group):
                h, b = divmod(i, 2)
                plan1.append((0, (r * half, (2 * h + b) * q), (r * half, (2 * h + 1 - b) * q)))
                pieces1.append(piece)
        w1, = place([(full, 4 * q)], pieces1, plan1, same)
        pieces2 = [a2, b2, fa2, fb2, na2, nb2, fna2, fnb2]
        plan2 = [(0, ((i // 2) * q, (i % 2) * half),) for i in range(8)]
        w2, = place([(4 * q, full)], pieces2, [(o, at, at) for o, at in plan2], same)

        flag = same.astype(jnp.int32).reshape(1)
        xw, = join(join_x_kernel, (xa, xb, xao, xbo), (full,), flag)
        far_part = gelu_call(xw, w1, mine, mine, [])
        s_0, s_1, *acts = gelu_call(xw, w1, mine, 0, far_part)
        v, = multi_mm([((0,), 0, False)], [xw], [wv_full], mine, 0, BF16)

        y_o, = multi_mm([((0, 1), 0, False)], acts, [w2], mine, mine, F32)
        y_r = over_core(y_o)
        g, = join(join_g_kernel, (ga, gb, gao, gbo), (full,))
        ya, yb = multi_mm([((0, 1), 0, False), ((2,), 1, False)],
            acts + [v], [w2, wo_full], mine, 0, BF16, split=2, add=y_r)
        y_out = cat(pair(y == 0, ya, over_y(yb)), 0)

        dacts = [token_call(dgelu_kernel, [g, (s_0, s_1)[h]], [(w2, q, h), (w2, q, 2 + h)], [(2 * q, BF16)], 2 * q)[0]
            for h in range(2)]

        dv, = multi_mm([((0,), 0, True)], [g], [wo_full], mine, 0, BF16)
        pv = dot_tn(xw[:mine], dv).reshape(2, 2, vrow, full)
        po = dot_tn(v, g[:mine]).reshape(2, 2, vrow, full)
        pv, po = lax.optimization_barrier((pv, po))
        pv_r = over_core(take(pv, 1 - c, 1, 1)[:, 0])
        po_r = over_core(take(po, 1 - c, 1, 1)[:, 0])
        pv, po = take(pv, c, 1, 1)[:, 0], take(po, c, 1, 1)[:, 0]
        r = over_y(take(pv, 1 - y, half, 2) + take(pv_r, 1 - y, half, 2))
        pv = take(pv, y, half, 2) + take(pv_r, y, half, 2) + r
        r = over_y(po[:, :, half:] + po_r[:, :, half:])
        po = po[:, :, :half] + po_r[:, :, :half] + r
        pv = pv[0] + over_x(pv[1])
        po = take(po, x, 1, 0)[0] + over_x(take(po, 1 - x, 1, 0)[0])
        grad_value = pv + over_z(pv)
        grad_output = po + over_z(po)

        s = dot_tn(acts[1], g)
        k = lax.optimization_barrier(dot_tn(acts[0], g))
        r1, r0 = over_x(s[q:]), over_x(s[:q])
        r = over_z(k[q:] + r1)
        k = lax.optimization_barrier(k)
        s = k[:q, half:] + r[:, half:] + r0[:, half:]
        down_mine = k[:q, :half] + r[:, :half] + r0[:, :half] + over_y(s)
        grad_down = cat(pair(z == 0, down_mine, over_z(down_mine)), 0)

        s = dot_tn(xw, dacts[1])
        k = lax.optimization_barrier(dot_tn(xw, dacts[0]))
        r1, r0 = over_z(s[half:]), over_z(s[:half])
        r = over_x(k[half:] + r1)
        s = lax.optimization_barrier(k)[:half] + r0
        keep, send = pair(same, s[:, :q] + r[:, q:], s[:, q:] + r[:, :q])
        s = keep + over_y(send)
        s_m = take(s, c, vrow, 0)
        s_o = over_core(take(s, 1 - c, vrow, 0))
        by_core = pair(c == 0, s_m, s_o)
        far = pair(c == 0, over_z(s_m), over_z(s_o))
        grad_up = cat([p for i in range(2) for p in pair(z == 0, by_core[i], far[i])], 1)

        x_o, = multi_mm([((0, 1), 0, True)], dacts, [w1], mine, mine, F32)
        x_r = over_core(x_o)
        da, db = multi_mm([((0, 1), 0, True), ((2,), 1, True)],
            dacts + [dv], [w1, wv_full], mine, 0, BF16, split=2, add=x_r)
        da, db = pair(same, da, db)
        grad_in = cat(pair(y == 0, da, over_y(db)), 0)
        return y_out, grad_in, grad_up, grad_down, grad_value, grad_output

    return jax.shard_map(
        device_step,
        mesh=mesh,
        in_specs=(act_spec, wgt_spec, wgt_spec, wgt_spec, wgt_spec, act_spec),
        out_specs=(act_spec, act_spec, wgt_spec, wgt_spec, wgt_spec, wgt_spec),
        check_vma=False,
    )
```
